32 devices in a mesh: depth: 8 (over z, core), tile: 4 (over y, x).
Axes of the slice: x: 2, y: 2, z: 4, core: 2. Of those that a mesh axis runs over, the one named last changes fastest.
Arguments:
- potential: float32 [8, 1024, 384], P('depth', 'tile'), may hold values from 0 to 3
- probe: bfloat16 [2, 256, 256], replicated, may hold values from -6 to 6
- positions: int32 [4, 19, 2], P('tile'), may hold values from 0 to 128
- intensity: bfloat16 [4, 4, 256, 256], P('tile'), may hold values from 0.099609375 to 3
- fwd_wave: float32 [8, 4, 2, 256, 256], P('depth', 'tile'), may hold values from -6 to 6
- adj_wave: bfloat16 [8, 4, 2, 256, 256], P('depth', 'tile'), may hold values from -6 to 6
- saved_wave: bfloat16 [8, 4, 4, 2, 256, 256], P('depth', 'tile'), may hold values from -6 to 6
Outputs:
- fwd_next: float32 [8, 4, 2, 256, 256], P('depth', 'tile')
- adj_next: bfloat16 [8, 4, 2, 256, 256], P('depth', 'tile')
- gradient: float32 [8, 1024, 384], P('depth', 'tile')
The draws below stay inside these ranges and needn't reach their ends.
Inputs may be any that keep to these rules, and one draw needn't show every extreme that they name: `positions`: window corners keep the whole window inside the tile's extent.
All inputs are finite; a program needn't handle non-finite values.
Results may differ from the reference program's by a relative error of at most 0.04.
Values may be sent and summed in bfloat16 or wider, within the bound.
A program may use at most 64 MiB of HBM per device.

```python
import math
import jax
import jax.numpy as jnp
from jax import lax

WAVE = 256
CORE = 256
MARGIN = 64
TICKS = 4
TILE = 384
SLICES = 8
WIDTH = 1024
MICRO = 19
N_DEPTH = 8
N_TILE = 4


def with_ends(drawn, own_key, low, high):
    spot = [jax.random.randint(jax.random.fold_in(own_key, axis), (), 0, length) for axis, length in enumerate(drawn.shape)]
    main_axis = drawn.shape.index(max(drawn.shape))
    next_to = spot[:main_axis] + [(spot[main_axis] + 1) % drawn.shape[main_axis]] + spot[main_axis + 1:]
    return drawn.at[tuple(spot)].set(low).at[tuple(next_to)].set(high)


def level_of(key, dims, shards, low, top_value):
    loudness = 1.0
    for dim, blocks in shards:
        draws = jax.random.uniform(jax.random.fold_in(jax.random.fold_in(key, 6), dim), (blocks,), jnp.float32, low / len(shards), top_value / len(shards))
        loudness = loudness * jnp.repeat(jnp.exp(draws), dims[dim] // blocks).reshape((-1,) + (1,) * (len(dims) - 1 - dim))
    return loudness


def noise(key, shape, scale, bound, cuts=(), kind=jnp.bfloat16):
    factor_of = level_of(key, shape, cuts, -0.22, 0.18) if cuts else 1.0
    entries = jax.random.normal(key, shape, jnp.float32) * scale * factor_of
    return jnp.minimum(jnp.maximum(entries, -bound), bound).astype(kind)


def setup_inputs(seed: int = 0) -> dict:
    key_of = jax.random.split(jax.random.key(seed), 8)
    return {
        "potential": jnp.clip(3.0 * jax.random.uniform(key_of[0], (SLICES, WIDTH, TILE), jnp.float32) ** level_of(key_of[0], (SLICES, WIDTH, TILE), ((0, 8), (1, 4)), -0.2, 0.2), 0.0, 3.0),
        "probe": noise(key_of[1], (2, WAVE, WAVE), 1.0, 6.0),
        "positions": with_ends(jax.random.randint(key_of[2], (N_TILE, MICRO, 2), 0, TILE - WAVE + 1), jax.random.fold_in(key_of[2], 1), 0, TILE - WAVE).astype(jnp.int32),
        "intensity": jnp.clip(jnp.exp(math.log(3.0) - 3.4051113 * jax.random.uniform(key_of[3], (N_TILE, TICKS, WAVE, WAVE), jnp.float32) ** level_of(key_of[3], (N_TILE, TICKS, WAVE, WAVE), ((0, 4),), -0.2, 0.2)), 0.099609375, 3.0).astype(jnp.bfloat16),
        "fwd_wave": noise(key_of[4], (SLICES, N_TILE, 2, WAVE, WAVE), 1.0, 6.0, ((0, 8), (1, 4)), jnp.float32),
        "adj_wave": noise(key_of[5], (SLICES, N_TILE, 2, WAVE, WAVE), 1.0, 6.0, ((0, 8), (1, 4))),
        "saved_wave": noise(key_of[6], (SLICES, N_TILE, TICKS, 2, WAVE, WAVE), 1.0, 6.0, ((0, 8), (1, 4))),
    }


SIGMA = 0.8
DEFOCUS = 6.0

def tables(n):
    idx = jnp.arange(n, dtype=jnp.int32)
    prod = idx[:, None] * idx[None, :] % n
    angle = prod.astype(jnp.float32) * (2.0 * math.pi / n)
    scale = 1.0 / math.sqrt(n)
    return ((jnp.cos(angle) * scale).astype(jnp.bfloat16), (jnp.sin(angle) * scale).astype(jnp.bfloat16))

def propagator(n):
    idx = jnp.arange(n, dtype=jnp.int32)
    freq = jnp.where(idx < n // 2, idx, idx - n).astype(jnp.float32)
    square = freq[:, None] * freq[:, None] + freq[None, :] * freq[None, :]
    phase = -math.pi * DEFOCUS * square / (n * n)
    return (jnp.cos(phase), jnp.sin(phase))

def to_half(value):
    return lax.optimization_barrier(value.astype(jnp.bfloat16)).astype(jnp.float32)

def product(left, right):
    return jnp.dot(left, right, precision=lax.Precision.HIGHEST)

def transform(real, imag, cos_t, sin_t, sign):
    xr = to_half(real)
    xi = to_half(imag)
    ar = product(cos_t, xr) + sign * product(sin_t, xi)
    ai = product(cos_t, xi) - sign * product(sin_t, xr)
    ar = to_half(ar)
    ai = to_half(ai)
    br = product(ar, cos_t) + sign * product(ai, sin_t)
    bi = product(ai, cos_t) - sign * product(ar, sin_t)
    return (br, bi)

def forward_section(wave, window, intens, is_last, cos_t, sin_t, prop_r, prop_i):
    trans_r = jnp.cos(SIGMA * window)
    trans_i = jnp.sin(SIGMA * window)
    ur = trans_r * wave[0] - trans_i * wave[1]
    ui = trans_r * wave[1] + trans_i * wave[0]
    big_r, big_i = transform(ur, ui, cos_t, sin_t, 1.0)
    far_r = big_r * prop_r - big_i * prop_i
    far_i = big_r * prop_i + big_i * prop_r
    excess = far_r * far_r + far_i * far_i - intens.astype(jnp.float32)
    src_r = jnp.where(is_last, excess * far_r, far_r)
    src_i = jnp.where(is_last, excess * far_i, far_i)
    out_r, out_i = transform(src_r, src_i, cos_t, sin_t, -1.0)
    return jnp.stack([out_r, out_i])

def backward_section(adjoint, saved, window, cos_t, sin_t, prop_r, prop_i):
    lr, li = transform(adjoint[0].astype(jnp.float32), adjoint[1].astype(jnp.float32), cos_t, sin_t, 1.0)
    mr = lr * prop_r + li * prop_i
    mi = li * prop_r - lr * prop_i
    lur, lui = transform(mr, mi, cos_t, sin_t, -1.0)
    trans_r = jnp.cos(SIGMA * window)
    trans_i = jnp.sin(SIGMA * window)
    saved_r = saved[0].astype(jnp.float32)
    saved_i = saved[1].astype(jnp.float32)
    uar = trans_r * saved_r - trans_i * saved_i
    uai = trans_r * saved_i + trans_i * saved_r
    delta = SIGMA * (lui * uar - lur * uai)
    back = jnp.stack([trans_r * lur + trans_i * lui, trans_r * lui - trans_i * lur])
    return (back, delta)

def reference(potential, probe, positions, intensity, fwd_wave, adj_wave, saved_wave):
    n = WAVE
    sections = N_DEPTH
    tiles = N_TILE
    core = CORE
    margin = MARGIN
    cos_h, sin_h = tables(n)
    cos_t = cos_h.astype(jnp.float32)
    sin_t = sin_h.astype(jnp.float32)
    prop_r, prop_i = propagator(n)
    padded = jnp.pad(potential, ((0, 0), (margin, margin), (0, 0)))
    section_ids = jnp.arange(sections, dtype=jnp.int32)
    last_mask = section_ids == sections - 1
    probe_wave = probe.astype(jnp.float32)

    def cut(extent, corner):
        return lax.dynamic_slice(extent, (corner[0], corner[1]), (n, n))

    def place(grad, delta, corner):
        old = lax.dynamic_slice(grad, (corner[0], corner[1]), (n, n))
        return lax.dynamic_update_slice(grad, old + delta, (corner[0], corner[1]))

    def one_tile(inputs):
        tile_index, spots, intens, wave, adjoint, saved = inputs
        start = (tile_index * core).astype(jnp.int32)
        extent = lax.dynamic_slice(padded, (jnp.int32(0), start, jnp.int32(0)), (sections, core + 2 * margin, TILE))
        grad = jnp.zeros((sections, core + 2 * margin, TILE), jnp.float32)
        for tick in range(TICKS):
            f_pos = spots[tick - section_ids + 2 * sections - 1]
            a_pos = spots[tick + section_ids]
            f_win = jax.vmap(cut)(extent, f_pos)
            a_win = jax.vmap(cut)(extent, a_pos)
            sent = jax.vmap(lambda w, v, last: forward_section(w, v, intens[tick], last, cos_t, sin_t, prop_r, prop_i))(wave, f_win, last_mask)
            back, delta = jax.vmap(lambda a, s, v: backward_section(a, s, v, cos_t, sin_t, prop_r, prop_i))(adjoint, saved[:, tick], a_win)
            grad = jax.vmap(place)(grad, delta, a_pos)
            wave = jnp.concatenate([probe_wave[None], sent[:-1]], 0)
            adjoint = jnp.concatenate([back[1:], sent[-1:]], 0).astype(jnp.bfloat16)
        return (wave, adjoint, grad)
    tile_ids = jnp.arange(tiles, dtype=jnp.int32)
    waves, adjoints, grads = lax.map(one_tile, (tile_ids, positions, intensity, jnp.swapaxes(fwd_wave, 0, 1), jnp.swapaxes(adj_wave, 0, 1), jnp.swapaxes(saved_wave, 0, 1)))
    inner = grads[:, :, margin:margin + core]
    zeros = jnp.zeros((1, sections, margin, TILE), jnp.float32)
    from_left = jnp.concatenate([zeros, grads[:-1, :, margin + core:]], 0)
    from_right = jnp.concatenate([grads[1:, :, :margin], zeros], 0)
    inner = inner + jnp.pad(from_left, ((0, 0), (0, 0), (0, core - margin), (0, 0)))
    inner = inner + jnp.pad(from_right, ((0, 0), (0, 0), (core - margin, 0), (0, 0)))
    gradient = jnp.swapaxes(inner, 0, 1).reshape(sections, tiles * core, TILE)
    return (jnp.swapaxes(waves, 0, 1), jnp.swapaxes(adjoints, 0, 1), gradient)
```

```python
import functools
import math

import jax
import jax.numpy as jnp
import numpy as np
from jax import lax
from jax.experimental import pallas as pl
from jax.experimental.pallas import tpu as pltpu
from jax.sharding import PartitionSpec as P

SIGMA = 0.8
DEFOCUS = 6.0
ROWS = 128
STEP = 32
MESH = pl.DeviceIdType.MESH
F32 = jnp.float32
BF16 = jnp.bfloat16


def tables(n):
    idx = np.arange(n)
    angle = (idx[:, None] * idx[None, :] % n) * (2.0 * math.pi / n)
    scale = 1.0 / math.sqrt(n)
    cos_t = np.asarray((np.cos(angle) * scale).astype(BF16)).astype(np.float64)
    sin_t = np.asarray((np.sin(angle) * scale).astype(BF16)).astype(np.float64)
    freq = np.where(idx < n // 2, idx, idx - n).astype(np.float64)
    q = np.exp(-1j * math.pi * DEFOCUS * freq * freq / (n * n))
    f = cos_t - 1j * sin_t
    m = (np.conj(f) * q[None, :]) @ f
    m = (m + m.T) / 2
    g = np.conj(f) * q[None, :]
    parts = (m.real, m.imag, cos_t, -sin_t, g.real, g.imag, g.T.real, g.T.imag)
    return np.stack([p.astype(BF16) for p in parts])


def sin_cos(x):
    k = jnp.floor(x * (2.0 / math.pi) + 0.5)
    r = x - k * 1.5703125
    r = r - k * 4.837512969970703125e-4
    r = r - k * 7.54978995489188216e-8
    z = r * r
    s = r + r * z * (-1.6666654611e-1 + z * (8.3321608736e-3 + z * -1.9515295891e-4))
    c = 1.0 - 0.5 * z + z * z * (
        4.166664568298827e-2 + z * (-1.388731625493765e-3 + z * 2.443315711809948e-5)
    )
    half = jnp.floor(k * 0.5)
    odd = k - 2.0 * half > 0.5
    quarter = half - 2.0 * jnp.floor(half * 0.5)
    sign = 1.0 - 2.0 * quarter
    sin_v = jnp.where(odd, c, s) * sign
    cos_v = jnp.where(odd, -s, c) * sign
    return sin_v, cos_v


def dot(a, b):
    return jnp.dot(a, b, preferred_element_type=F32)


def kernel(
    sections, tiles,
    pos, pot, probe, inten, fwd, adj, saved, tab,
    o_fwd, o_adj, o_grad,
    in_f, in_b, out_f, out_b, l_f, r_f, l_b, r_b, l_g, r_g,
    ext, tf, ta, bk, total, a_buf, y_buf,
    halo_out, halo_in, edge_out, edge_in,
    send_f, recv_f, send_b, recv_b, send_h, recv_h, send_e, recv_e,
):
    n = probe.shape[1]
    nc = n // ROWS
    core, width = pot.shape[1], pot.shape[2]
    margin = (width - core) // 2
    ticks = inten.shape[1]
    s = lax.axis_index("depth")
    t = lax.axis_index("tile")
    first, last = s == 0, s == sections - 1
    low, high = t == 0, t == tiles - 1

    barrier = pltpu.get_barrier_semaphore()
    one = lambda c: jnp.where(c, 1, 0).astype(jnp.int32)

    def greet(cond, axis, to):
        @pl.when(cond)
        def _():
            pl.semaphore_signal(barrier, inc=1, device_id={axis: to}, device_id_type=MESH)

    greet(s > 0, "depth", s - 1)
    greet(s < sections - 1, "depth", s + 1)
    greet(t > 0, "tile", t - 1)
    greet(t < tiles - 1, "tile", t + 1)
    halo_out[0] = pot[0, 0:margin, :].astype(BF16)
    halo_out[1] = pot[0, core - margin : core, :].astype(BF16)
    pl.semaphore_wait(barrier, one(s > 0) + one(s < sections - 1) + one(t > 0) + one(t < tiles - 1))

    def hop(src, dst, ssem, rsem, axis, to):
        return pltpu.make_async_remote_copy(
            src_ref=src, dst_ref=dst, send_sem=ssem, recv_sem=rsem,
            device_id={axis: to}, device_id_type=MESH,
        )

    def tile_pair(src, dst, ssem, rsem):
        down = hop(src.at[0], dst.at[1], ssem.at[0], rsem.at[1], "tile", t - 1)
        up = hop(src.at[1], dst.at[0], ssem.at[1], rsem.at[0], "tile", t + 1)
        return down, up

    def tile_start(src, dst, ssem, rsem):
        down, up = tile_pair(src, dst, ssem, rsem)
        pl.when(t > 0)(down.start)
        pl.when(t < tiles - 1)(up.start)

    def tile_wait(src, dst, ssem, rsem):
        down, up = tile_pair(src, dst, ssem, rsem)

        @pl.when(t > 0)
        def _():
            down.wait_send()
            up.wait_recv()

        @pl.when(t < tiles - 1)
        def _():
            up.wait_send()
            down.wait_recv()

    tile_start(halo_out, halo_in, send_h, recv_h)

    def fill(l_ref, r_ref, lr, li, rr, ri):
        for c in range(nc):
            cols = slice(c * ROWS, (c + 1) * ROWS)
            l_ref[c, 0:n, 0:ROWS] = lr[:, cols]
            l_ref[c, 0:n, ROWS : 2 * ROWS] = -li[:, cols]
            l_ref[c, n : 2 * n, 0:ROWS] = li[:, cols]
            l_ref[c, n : 2 * n, ROWS : 2 * ROWS] = lr[:, cols]
        r_ref[0:n, 0:n] = rr
        r_ref[0:n, n : 2 * n] = ri
        r_ref[n : 2 * n, 0:n] = -ri
        r_ref[n : 2 * n, n : 2 * n] = rr

    fill(l_b, r_b, tab[0], -tab[1], tab[0], -tab[1])

    @pl.when(jnp.logical_not(last))
    def _():
        fill(l_f, r_f, tab[0], tab[1], tab[0], tab[1])

    @pl.when(last)
    def _():
        fill(l_f, r_f, tab[2], tab[3], tab[2], tab[3])
        fill(l_g, r_g, tab[4], tab[5], tab[6], tab[7])

    for c in range(nc):
        for part in range(2):
            rows = slice(c * ROWS, (c + 1) * ROWS)
            to = slice(part * ROWS, (part + 1) * ROWS)
            in_f[0, c, to, :] = fwd[0, 0, part, rows, :].astype(BF16)
            in_b[0, c, to, :] = adj[0, 0, part, rows, :]

    @pl.when(first)
    def _():
        for k in range(ticks):
            for c in range(nc):
                in_f[k + 1, c] = jnp.concatenate(
                    [probe[part, c * ROWS : (c + 1) * ROWS, :] for part in range(2)], axis=0
                )

    total[...] = jnp.zeros_like(total)
    ext[margin : margin + core, :] = pot[0].astype(BF16)

    @pl.when(low)
    def _():
        halo_in[0] = jnp.zeros((margin, width), BF16)
        edge_in[0] = jnp.zeros((margin, width), BF16)

    @pl.when(high)
    def _():
        halo_in[1] = jnp.zeros((margin, width), BF16)
        edge_in[1] = jnp.zeros((margin, width), BF16)

    tile_wait(halo_out, halo_in, send_h, recv_h)
    ext[0:margin, :] = halo_in[0]
    ext[margin + core :, :] = halo_in[1]

    def chosen(offset, axis):
        shape = (n, width) if axis else (width, n)
        ahead = lax.broadcasted_iota(jnp.int32, shape, axis) - lax.broadcasted_iota(
            jnp.int32, shape, 1 - axis
        )
        return jnp.where(ahead == offset, 1.0, 0.0).astype(BF16)

    def window(index, out):
        rows = dot(chosen(pos[0, index, 0], 1), ext[...]).astype(BF16)
        bk[0] = SIGMA * dot(rows, chosen(pos[0, index, 1], 0))
        for at in range(0, n, STEP):
            sv, cv = sin_cos(bk[0, at : at + STEP, :])
            out[0, at : at + STEP, :] = cv
            out[1, at : at + STEP, :] = sv

    def copy_f(k, c):
        return hop(out_f.at[k, c], in_f.at[k + 1, c], send_f.at[k, c], recv_f.at[k, c], "depth", s + 1)

    def copy_b(k, c):
        return hop(out_b.at[k, c], in_b.at[k + 1, c], send_b.at[k, c], recv_b.at[k, c], "depth", s - 1)

    def right(r_ref, c):
        rows = slice(c * ROWS, (c + 1) * ROWS)
        more = slice(n + c * ROWS, n + (c + 1) * ROWS)
        return dot(jnp.concatenate([a_buf[rows, :], a_buf[more, :]], axis=1), r_ref[...])

    def tick(k, carry):
        window(k + s, ta)
        window(k - s + 2 * sections - 1, tf)
        acc = None
        for c in range(nc):
            @pl.when(jnp.logical_and(k > 0, jnp.logical_not(last)))
            def _():
                copy_b(k - 1, c).wait_recv()
            term = dot(l_b[c], in_b[k, c])
            acc = term if acc is None else acc + term
        a_buf[...] = acc.astype(BF16)
        for c in range(nc):
            rows = slice(c * ROWS, (c + 1) * ROWS)
            lu = right(r_b, c)
            lur, lui = lu[:, 0:n], lu[:, n : 2 * n]
            tr, ti = ta[0, rows, :], ta[1, rows, :]
            br = tr * lur + ti * lui
            bi = tr * lui - ti * lur
            bk[0, rows, :] = br
            bk[1, rows, :] = bi
            out_b[k, c, 0:ROWS, :] = br.astype(BF16)
            out_b[k, c, ROWS : 2 * ROWS, :] = bi.astype(BF16)

            @pl.when(jnp.logical_not(first))
            def _():
                copy_b(k, c).start()
        acc = None
        for c in range(nc):
            rows = slice(c * ROWS, (c + 1) * ROWS)

            @pl.when(jnp.logical_and(k > 0, jnp.logical_not(first)))
            def _():
                copy_f(k - 1, c).wait_recv()
            wr = in_f[k, c, 0:ROWS, :].astype(F32)
            wi = in_f[k, c, ROWS : 2 * ROWS, :].astype(F32)
            tr, ti = tf[0, rows, :], tf[1, rows, :]
            u = jnp.concatenate([tr * wr - ti * wi, tr * wi + ti * wr], axis=0).astype(BF16)
            term = dot(l_f[c], u)
            acc = term if acc is None else acc + term
        a_buf[...] = acc.astype(BF16)

        @pl.when(jnp.logical_not(last))
        def _():
            for c in range(nc):
                out = right(r_f, c)
                out_f[k, c, 0:ROWS, :] = out[:, 0:n].astype(BF16)
                out_f[k, c, ROWS : 2 * ROWS, :] = out[:, n : 2 * n].astype(BF16)
                copy_f(k, c).start()

        @pl.when(last)
        def _():
            for c in range(nc):
                rows = slice(c * ROWS, (c + 1) * ROWS)
                out = right(r_f, c)
                vr, vi = out[:, 0:n], out[:, n : 2 * n]
                excess = vr * vr + vi * vi - inten[0, k, rows, :].astype(F32)
                y_buf[c, 0:ROWS, :] = (excess * vr).astype(BF16)
                y_buf[c, ROWS : 2 * ROWS, :] = (excess * vi).astype(BF16)
            left = None
            for c in range(nc):
                term = dot(l_g[c], y_buf[c])
                left = term if left is None else left + term
            a_buf[...] = left.astype(BF16)
            for c in range(nc):
                out = right(r_g, c)
                in_b[k + 1, c, 0:ROWS, :] = out[:, 0:n].astype(BF16)
                in_b[k + 1, c, ROWS : 2 * ROWS, :] = out[:, n : 2 * n].astype(BF16)

        sr = saved[0, 0, k, 0].astype(F32)
        si = saved[0, 0, k, 1].astype(F32)
        delta = SIGMA * (bk[1] * sr - bk[0] * si)
        coarse = delta.astype(BF16)
        fine = (delta - coarse.astype(F32)).astype(BF16)
        tall = dot(chosen(pos[0, k + s, 0], 0), jnp.concatenate([coarse, fine], axis=1)).astype(BF16)
        across = chosen(pos[0, k + s, 1], 1)
        total[...] += dot(tall[:, 0:n], across) + dot(tall[:, n : 2 * n], across)
        return carry

    lax.fori_loop(0, ticks, tick, 0)

    edge_out[0] = total[0:margin, :].astype(BF16)
    edge_out[1] = total[margin + core :, :].astype(BF16)
    tile_start(edge_out, edge_in, send_e, recv_e)
    o_grad[0, margin : core - margin, :] = total[2 * margin : core, :]
    tile_wait(edge_out, edge_in, send_e, recv_e)
    o_grad[0, 0:margin, :] = total[margin : 2 * margin, :] + edge_in[0].astype(F32)
    o_grad[0, core - margin : core, :] = total[core : core + margin, :] + edge_in[1].astype(F32)
    for c in range(nc):
        rows = slice(c * ROWS, (c + 1) * ROWS)

        @pl.when(jnp.logical_not(last))
        def _():
            copy_b(ticks - 1, c).wait_recv()
        o_adj[0, 0, 0, rows, :] = in_b[ticks, c, 0:ROWS, :]
        o_adj[0, 0, 1, rows, :] = in_b[ticks, c, ROWS : 2 * ROWS, :]

        @pl.when(jnp.logical_not(first))
        def _():
            copy_f(ticks - 1, c).wait_recv()
        o_fwd[0, 0, 0, rows, :] = in_f[ticks, c, 0:ROWS, :].astype(F32)
        o_fwd[0, 0, 1, rows, :] = in_f[ticks, c, ROWS : 2 * ROWS, :].astype(F32)
    for k in range(ticks):
        for c in range(nc):
            @pl.when(jnp.logical_not(last))
            def _():
                copy_f(k, c).wait_send()

            @pl.when(jnp.logical_not(first))
            def _():
                copy_b(k, c).wait_send()


def on_device(sections, tiles, potential, probe, positions, intensity, fwd_wave, adj_wave, saved_wave):
    n = probe.shape[1]
    nc = n // ROWS
    ticks = intensity.shape[1]
    core, width = potential.shape[1], potential.shape[2]
    margin = (width - core) // 2
    vmem = pl.BlockSpec(memory_space=pltpu.VMEM)
    smem = pl.BlockSpec(memory_space=pltpu.SMEM)
    dma = lambda *shape: pltpu.SemaphoreType.DMA(shape)
    wave = lambda count: pltpu.VMEM((count, nc, 2 * ROWS, n), BF16)
    lt = pltpu.VMEM((nc, 2 * n, 2 * ROWS), BF16)
    rt = pltpu.VMEM((2 * n, 2 * n), BF16)
    two = pltpu.VMEM((2, n, n), F32)
    strip = pltpu.VMEM((2, margin, width), BF16)
    return pl.pallas_call(
        functools.partial(kernel, sections, tiles),
        out_shape=(
            jax.ShapeDtypeStruct(fwd_wave.shape, F32),
            jax.ShapeDtypeStruct(adj_wave.shape, BF16),
            jax.ShapeDtypeStruct(potential.shape, F32),
        ),
        in_specs=[smem] + [vmem] * 7,
        out_specs=(vmem, vmem, vmem),
        scratch_shapes=[
            wave(ticks + 1), wave(ticks + 1), wave(ticks), wave(ticks),
            lt, rt, lt, rt, lt, rt,
            pltpu.VMEM((width, width), BF16), two, two, two,
            pltpu.VMEM((width, width), F32),
            pltpu.VMEM((2 * n, n), BF16),
            pltpu.VMEM((nc, 2 * ROWS, n), BF16),
            strip, strip, strip, strip,
            dma(ticks, nc), dma(ticks, nc), dma(ticks, nc), dma(ticks, nc),
            dma(2), dma(2), dma(2), dma(2),
        ],
        compiler_params=pltpu.CompilerParams(
            collective_id=0, has_side_effects=True, vmem_limit_bytes=60 * 1024 * 1024
        ),
        name="window",
    )(positions, potential, probe, intensity, fwd_wave, adj_wave, saved_wave, jnp.asarray(tables(n)))


def solution(mesh):
    placed = (
        P("depth", "tile", None),
        P(),
        P("tile", None, None),
        P("tile", None, None, None),
        P("depth", "tile", None, None, None),
        P("depth", "tile", None, None, None),
        P("depth", "tile", None, None, None, None),
    )
    return jax.shard_map(
        functools.partial(on_device, mesh.shape["depth"], mesh.shape["tile"]),
        mesh=mesh,
        in_specs=placed,
        out_specs=(
            P("depth", "tile", None, None, None),
            P("depth", "tile", None, None, None),
            P("depth", "tile", None),
        ),
        check_vma=False,
    )
```

```python
import functools
import math

import jax
import jax.numpy as jnp
import numpy as np
from jax import lax
from jax.experimental import pallas as pl
from jax.experimental.pallas import tpu as pltpu
from jax.sharding import PartitionSpec as P

SIGMA = 0.8
DEFOCUS = 6.0
ROWS = 128
STEP = 32
VLIM = 55
MESH = pl.DeviceIdType.MESH
F32 = jnp.float32
BF16 = jnp.bfloat16


def rounded(x):
    return x.real.astype(BF16).astype(np.float64) + 1j * x.imag.astype(BF16).astype(np.float64)


def tables(n):
    idx = np.arange(n)
    angle = (idx[:, None] * idx[None, :] % n) * (2.0 * math.pi / n)
    scale = 1.0 / math.sqrt(n)
    cos_t = np.asarray((np.cos(angle) * scale).astype(BF16)).astype(np.float64)
    sin_t = np.asarray((np.sin(angle) * scale).astype(BF16)).astype(np.float64)
    freq = np.where(idx < n // 2, idx, idx - n).astype(np.float64)
    q = np.exp(-1j * math.pi * DEFOCUS * freq * freq / (n * n))
    f = cos_t - 1j * sin_t
    m = (np.conj(f) * q[None, :]) @ f
    m = (m + m.T) / 2
    best = (np.inf, 1.0)
    for size in np.linspace(0.7, 1.4, 64):
        turns = size * np.exp(1j * np.linspace(0.0, math.pi / 2, 128, endpoint=False))
        row = m[0][None, :] / turns[:, None]
        miss = np.sum(np.abs(rounded(row) - row) ** 2, axis=1) * size * size
        at = int(np.argmin(miss))
        if miss[at] < best[0]:
            best = (miss[at], turns[at])
    z = best[1]
    near = rounded(z * m)
    rest = z * m - near
    g = np.conj(f) * q[None, :]
    parts = [x for v in (near, rest, m / z, f, g, g.T) for x in (v.real, v.imag)]
    return np.stack([p.astype(BF16) for p in parts])


def sin_cos(x):
    k = jnp.floor(x * (2.0 / math.pi) + 0.5)
    r = x - k * 1.5703125
    r = r - k * 4.837512969970703125e-4
    r = r - k * 7.54978995489188216e-8
    z = r * r
    s = r + r * z * (-1.6666654611e-1 + z * (8.3321608736e-3 + z * -1.9515295891e-4))
    c = 1.0 - 0.5 * z + z * z * (
        4.166664568298827e-2 + z * (-1.388731625493765e-3 + z * 2.443315711809948e-5)
    )
    half = jnp.floor(k * 0.5)
    odd = k - 2.0 * half > 0.5
    quarter = half - 2.0 * jnp.floor(half * 0.5)
    sign = 1.0 - 2.0 * quarter
    sin_v = jnp.where(odd, c, s) * sign
    cos_v = jnp.where(odd, -s, c) * sign
    return sin_v, cos_v


def dot(a, b):
    return jnp.dot(a, b, preferred_element_type=F32)


def kernel(
    sections, tiles,
    pos, pot_h, probe_h, inten_h, fwd_h, adj_h, saved_h, tab_h,
    o_fwd, o_adj, o_grad,
    in_f, in_b, out_f, out_b, l_f, m_f, r_f, l_b, m_b, r_b, l_g, r_g,
    ext, tf, ta, bk, total, a_buf, y_buf,
    halo_out, halo_in, edge_out, edge_in,
    pot, probe, inten, fwd, adj, saved, tab, load_sem,
    send_f, recv_f, send_b, recv_b, send_h, recv_h, send_e, recv_e,
):
    n = probe.shape[1]
    nc = n // ROWS
    core, width = pot.shape[1], pot.shape[2]
    margin = (width - core) // 2
    ticks = inten.shape[1]
    s = lax.axis_index("depth")
    t = lax.axis_index("tile")
    first, last = s == 0, s == sections - 1
    low, high = t == 0, t == tiles - 1

    loads = {}
    for i, (name, src, dst) in enumerate((
        ("pot", pot_h, pot), ("tab", tab_h, tab), ("adj", adj_h, adj), ("fwd", fwd_h, fwd),
        ("probe", probe_h, probe), ("saved", saved_h, saved), ("inten", inten_h, inten),
    )):
        loads[name] = pltpu.make_async_copy(src, dst, load_sem.at[i])
        loads[name].start()

    barrier = pltpu.get_barrier_semaphore()
    one = lambda c: jnp.where(c, 1, 0).astype(jnp.int32)

    def greet(cond, axis, to):
        @pl.when(cond)
        def _():
            pl.semaphore_signal(barrier, inc=1, device_id={axis: to}, device_id_type=MESH)

    greet(s > 0, "depth", s - 1)
    greet(s < sections - 1, "depth", s + 1)
    greet(t > 0, "tile", t - 1)
    greet(t < tiles - 1, "tile", t + 1)
    loads["pot"].wait()
    halo_out[0] = pot[0, 0:margin, :].astype(BF16)
    halo_out[1] = pot[0, core - margin : core, :].astype(BF16)
    pl.semaphore_wait(barrier, one(s > 0) + one(s < sections - 1) + one(t > 0) + one(t < tiles - 1))

    def hop(src, dst, ssem, rsem, axis, to):
        return pltpu.make_async_remote_copy(
            src_ref=src, dst_ref=dst, send_sem=ssem, recv_sem=rsem,
            device_id={axis: to}, device_id_type=MESH,
        )

    def tile_pair(src, dst, ssem, rsem):
        down = hop(src.at[0], dst.at[1], ssem.at[0], rsem.at[1], "tile", t - 1)
        up = hop(src.at[1], dst.at[0], ssem.at[1], rsem.at[0], "tile", t + 1)
        return down, up

    def tile_start(src, dst, ssem, rsem):
        down, up = tile_pair(src, dst, ssem, rsem)
        pl.when(t > 0)(down.start)
        pl.when(t < tiles - 1)(up.start)

    def tile_wait(src, dst, ssem, rsem):
        down, up = tile_pair(src, dst, ssem, rsem)

        @pl.when(t > 0)
        def _():
            down.wait_send()
            up.wait_recv()

        @pl.when(t < tiles - 1)
        def _():
            up.wait_send()
            down.wait_recv()

    tile_start(halo_out, halo_in, send_h, recv_h)

    def fill_left(ref, lr, li):
        for c in range(nc):
            cols = slice(c * ROWS, (c + 1) * ROWS)
            ref[c, 0:n, 0:ROWS] = lr[:, cols]
            ref[c, 0:n, ROWS : 2 * ROWS] = -li[:, cols]
            ref[c, n : 2 * n, 0:ROWS] = li[:, cols]
            ref[c, n : 2 * n, ROWS : 2 * ROWS] = lr[:, cols]

    def fill_right(ref, rr, ri):
        ref[0:n, 0:n] = rr
        ref[0:n, n : 2 * n] = ri
        ref[n : 2 * n, 0:n] = -ri
        ref[n : 2 * n, n : 2 * n] = rr

    loads["tab"].wait()
    fill_left(l_b, tab[0], -tab[1])
    fill_left(m_b, tab[2], -tab[3])
    fill_right(r_b, tab[4], -tab[5])

    @pl.when(jnp.logical_not(last))
    def _():
        fill_left(l_f, tab[0], tab[1])
        fill_left(m_f, tab[2], tab[3])
        fill_right(r_f, tab[4], tab[5])

    @pl.when(last)
    def _():
        fill_left(l_f, tab[6], tab[7])
        m_f[...] = jnp.zeros_like(m_f)
        fill_right(r_f, tab[6], tab[7])
        fill_left(l_g, tab[8], tab[9])
        fill_right(r_g, tab[10], tab[11])

    for name in ("adj", "fwd", "probe"):
        loads[name].wait()
    for c in range(nc):
        for part in range(2):
            rows = slice(c * ROWS, (c + 1) * ROWS)
            to = slice(part * ROWS, (part + 1) * ROWS)
            in_f[0, c, to, :] = fwd[0, 0, part, rows, :].astype(BF16)
            in_b[0, c, to, :] = adj[0, 0, part, rows, :]

    @pl.when(first)
    def _():
        for k in range(ticks):
            for c in range(nc):
                in_f[k + 1, c] = jnp.concatenate(
                    [probe[part, c * ROWS : (c + 1) * ROWS, :] for part in range(2)], axis=0
                )

    total[...] = jnp.zeros_like(total)
    ext[margin : margin + core, :] = pot[0].astype(BF16)

    @pl.when(low)
    def _():
        halo_in[0] = jnp.zeros((margin, width), BF16)
        edge_in[0] = jnp.zeros((margin, width), BF16)

    @pl.when(high)
    def _():
        halo_in[1] = jnp.zeros((margin, width), BF16)
        edge_in[1] = jnp.zeros((margin, width), BF16)

    tile_wait(halo_out, halo_in, send_h, recv_h)
    ext[0:margin, :] = halo_in[0]
    ext[margin + core :, :] = halo_in[1]

    def chosen(offset, axis):
        shape = (n, width) if axis else (width, n)
        ahead = lax.broadcasted_iota(jnp.int32, shape, axis) - lax.broadcasted_iota(
            jnp.int32, shape, 1 - axis
        )
        return jnp.where(ahead == offset, 1.0, 0.0).astype(BF16)

    def window(index, out):
        rows = dot(chosen(pos[0, 0, index], 1), ext[...]).astype(BF16)
        bk[0] = SIGMA * dot(rows, chosen(pos[0, 1, index], 0))
        for at in range(0, n, STEP):
            sv, cv = sin_cos(bk[0, at : at + STEP, :])
            out[0, at : at + STEP, :] = cv
            out[1, at : at + STEP, :] = sv

    def copy_f(k, c):
        return hop(out_f.at[k, c], in_f.at[k + 1, c], send_f.at[k, c], recv_f.at[k, c], "depth", s + 1)

    def copy_b(k, c):
        return hop(out_b.at[k, c], in_b.at[k + 1, c], send_b.at[k, c], recv_b.at[k, c], "depth", s - 1)

    def right(r_ref, c):
        rows = slice(c * ROWS, (c + 1) * ROWS)
        more = slice(n + c * ROWS, n + (c + 1) * ROWS)
        return dot(jnp.concatenate([a_buf[rows, :], a_buf[more, :]], axis=1), r_ref[...])

    def backward(k):
        acc = None
        for c in range(nc):
            @pl.when(jnp.logical_and(k > 0, jnp.logical_not(last)))
            def _():
                copy_b(k - 1, c).wait_recv()
            term = dot(l_b[c], in_b[k, c]) + dot(m_b[c], in_b[k, c])
            acc = term if acc is None else acc + term
        a_buf[...] = acc.astype(BF16)
        for c in range(nc):
            rows = slice(c * ROWS, (c + 1) * ROWS)
            lu = right(r_b, c)
            lur, lui = lu[:, 0:n], lu[:, n : 2 * n]
            tr, ti = ta[0, rows, :], ta[1, rows, :]
            br = tr * lur + ti * lui
            bi = tr * lui - ti * lur
            bk[0, rows, :] = br
            bk[1, rows, :] = bi
            out_b[k, c, 0:ROWS, :] = br.astype(BF16)
            out_b[k, c, ROWS : 2 * ROWS, :] = bi.astype(BF16)

            @pl.when(jnp.logical_not(first))
            def _():
                copy_b(k, c).start()

    def forward(k):
        acc = None
        for c in range(nc):
            rows = slice(c * ROWS, (c + 1) * ROWS)

            @pl.when(jnp.logical_and(k > 0, jnp.logical_not(first)))
            def _():
                copy_f(k - 1, c).wait_recv()
            wr = in_f[k, c, 0:ROWS, :].astype(F32)
            wi = in_f[k, c, ROWS : 2 * ROWS, :].astype(F32)
            tr, ti = tf[0, rows, :], tf[1, rows, :]
            u = jnp.concatenate([tr * wr - ti * wi, tr * wi + ti * wr], axis=0).astype(BF16)
            term = dot(l_f[c], u) + dot(m_f[c], u)
            acc = term if acc is None else acc + term
        a_buf[...] = acc.astype(BF16)

        @pl.when(jnp.logical_not(last))
        def _():
            for c in range(nc):
                out = right(r_f, c)
                out_f[k, c, 0:ROWS, :] = out[:, 0:n].astype(BF16)
                out_f[k, c, ROWS : 2 * ROWS, :] = out[:, n : 2 * n].astype(BF16)
                copy_f(k, c).start()

        @pl.when(last)
        def _():
            for c in range(nc):
                rows = slice(c * ROWS, (c + 1) * ROWS)
                out = right(r_f, c)
                vr, vi = out[:, 0:n], out[:, n : 2 * n]
                excess = vr * vr + vi * vi - inten[0, k, rows, :].astype(F32)
                y_buf[c, 0:ROWS, :] = (excess * vr).astype(BF16)
                y_buf[c, ROWS : 2 * ROWS, :] = (excess * vi).astype(BF16)
            left = None
            for c in range(nc):
                term = dot(l_g[c], y_buf[c])
                left = term if left is None else left + term
            a_buf[...] = left.astype(BF16)
            for c in range(nc):
                out = right(r_g, c)
                in_b[k + 1, c, 0:ROWS, :] = out[:, 0:n].astype(BF16)
                in_b[k + 1, c, ROWS : 2 * ROWS, :] = out[:, n : 2 * n].astype(BF16)

    early = jnp.logical_or(first, jnp.logical_and(lax.rem(s, 2) == 1, jnp.logical_not(last)))

    def tick(k, carry):
        window(k + s, ta)
        window(k - s + 2 * sections - 1, tf)

        @pl.when(early)
        def _():
            forward(k)

        backward(k)

        @pl.when(jnp.logical_not(early))
        def _():
            forward(k)

        sr = saved[0, 0, k, 0].astype(F32)
        si = saved[0, 0, k, 1].astype(F32)
        delta = SIGMA * (bk[1] * sr - bk[0] * si)
        coarse = delta.astype(BF16)
        fine = (delta - coarse.astype(F32)).astype(BF16)
        tall = dot(chosen(pos[0, 0, k + s], 0), jnp.concatenate([coarse, fine], axis=1)).astype(BF16)
        across = chosen(pos[0, 1, k + s], 1)
        total[...] += dot(tall[:, 0:n], across) + dot(tall[:, n : 2 * n], across)
        return carry

    for name in ("saved", "inten"):
        loads[name].wait()
    lax.fori_loop(0, ticks, tick, 0)

    edge_out[0] = total[0:margin, :].astype(BF16)
    edge_out[1] = total[margin + core :, :].astype(BF16)
    tile_start(edge_out, edge_in, send_e, recv_e)
    o_grad[0, margin : core - margin, :] = total[2 * margin : core, :]
    tile_wait(edge_out, edge_in, send_e, recv_e)
    o_grad[0, 0:margin, :] = total[margin : 2 * margin, :] + edge_in[0].astype(F32)
    o_grad[0, core - margin : core, :] = total[core : core + margin, :] + edge_in[1].astype(F32)
    for c in range(nc):
        rows = slice(c * ROWS, (c + 1) * ROWS)

        @pl.when(jnp.logical_not(last))
        def _():
            copy_b(ticks - 1, c).wait_recv()
        o_adj[0, 0, 0, rows, :] = in_b[ticks, c, 0:ROWS, :]
        o_adj[0, 0, 1, rows, :] = in_b[ticks, c, ROWS : 2 * ROWS, :]

        @pl.when(jnp.logical_not(first))
        def _():
            copy_f(ticks - 1, c).wait_recv()
        o_fwd[0, 0, 0, rows, :] = in_f[ticks, c, 0:ROWS, :]
        o_fwd[0, 0, 1, rows, :] = in_f[ticks, c, ROWS : 2 * ROWS, :]
    for k in range(ticks):
        for c in range(nc):
            @pl.when(jnp.logical_not(last))
            def _():
                copy_f(k, c).wait_send()

            @pl.when(jnp.logical_not(first))
            def _():
                copy_b(k, c).wait_send()


def on_device(sections, tiles, potential, probe, positions, intensity, fwd_wave, adj_wave, saved_wave):
    n = probe.shape[1]
    nc = n // ROWS
    ticks = intensity.shape[1]
    core, width = potential.shape[1], potential.shape[2]
    margin = (width - core) // 2
    tab = jnp.asarray(tables(n))
    held = lambda x: pltpu.VMEM(x.shape, x.dtype)
    vmem = pl.BlockSpec(memory_space=pltpu.VMEM)
    smem = pl.BlockSpec(memory_space=pltpu.SMEM)
    dma = lambda *shape: pltpu.SemaphoreType.DMA(shape)
    wave = lambda count: pltpu.VMEM((count, nc, 2 * ROWS, n), BF16)
    lt = pltpu.VMEM((nc, 2 * n, 2 * ROWS), BF16)
    rt = pltpu.VMEM((2 * n, 2 * n), BF16)
    two = pltpu.VMEM((2, n, n), F32)
    strip = pltpu.VMEM((2, margin, width), BF16)
    wave_next, adj_next, gradient = pl.pallas_call(
        functools.partial(kernel, sections, tiles),
        out_shape=(
            jax.ShapeDtypeStruct(fwd_wave.shape, BF16),
            jax.ShapeDtypeStruct(adj_wave.shape, BF16),
            jax.ShapeDtypeStruct(potential.shape, F32),
        ),
        in_specs=[smem] + [pl.BlockSpec(memory_space=pltpu.HBM)] * 7,
        out_specs=(vmem, vmem, vmem),
        scratch_shapes=[
            wave(ticks + 1), wave(ticks + 1), wave(ticks), wave(ticks),
            lt, lt, rt, lt, lt, rt, lt, rt,
            pltpu.VMEM((width, width), BF16), two, two, two,
            pltpu.VMEM((width, width), F32),
            pltpu.VMEM((2 * n, n), BF16),
            pltpu.VMEM((nc, 2 * ROWS, n), BF16),
            strip, strip, strip, strip,
            held(potential), held(probe), held(intensity), held(fwd_wave), held(adj_wave),
            held(saved_wave), held(tab), dma(7),
            dma(ticks, nc), dma(ticks, nc), dma(ticks, nc), dma(ticks, nc),
            dma(2), dma(2), dma(2), dma(2),
        ],
        compiler_params=pltpu.CompilerParams(
            collective_id=0, has_side_effects=True, vmem_limit_bytes=VLIM * 1024 * 1024
        ),
        name="window",
    )(jnp.swapaxes(positions, 1, 2), potential, probe, intensity, fwd_wave, adj_wave, saved_wave, tab)
    return wave_next.astype(F32), adj_next, gradient


def solution(mesh):
    placed = (
        P("depth", "tile", None),
        P(),
        P("tile", None, None),
        P("tile", None, None, None),
        P("depth", "tile", None, None, None),
        P("depth", "tile", None, None, None),
        P("depth", "tile", None, None, None, None),
    )
    return jax.shard_map(
        functools.partial(on_device, mesh.shape["depth"], mesh.shape["tile"]),
        mesh=mesh,
        in_specs=placed,
        out_specs=(
            P("depth", "tile", None, None, None),
            P("depth", "tile", None, None, None),
            P("depth", "tile", None),
        ),
        check_vma=False,
    )
```
